128 devices in a mesh: layer: 4 (over z_hi, core), dp: 32 (over y, z_lo, x).
Axes of the slice: x: 4, y: 4, z: 4 (z_hi: 2, z_lo: 2; z = z_hi * 2 + z_lo), core: 2. Of those that a mesh axis runs over, the one named last changes fastest.
Arguments:
- out_grads: bfloat16 [4, 128, 16384], P('layer', None, 'dp'), may hold values from -3 to 3
- in_acts: bfloat16 [4, 128, 4096], P('layer', None, 'dp'), may hold values from -3 to 3
- out_basis: bfloat16 [4, 16384, 16384], P('layer', None, 'dp'), may hold values from -0.046875 to 0.046875
- in_basis: bfloat16 [4, 4096, 4096], P('layer', None, 'dp'), may hold values from -0.09375 to 0.09375
- eigenvalues: bfloat16 [4, 16384, 4096], P('layer', 'dp'), may hold values from 0.5 to 50
- out_store: bfloat16 [4, 64, 32, 16384], P('layer', 'dp'), may hold values from -0.046875 to 0.046875
- in_store: bfloat16 [4, 64, 32, 4096], P('layer', 'dp'), may hold values from -0.09375 to 0.09375
- counts: int32 [64], P('dp'), may hold values from 1 to 4096
- winners: int32 [4, 6], replicated, may hold values from 0 to 63
Outputs:
- influence: float32 [4, 6, 32], replicated
The draws below stay inside these ranges and needn't reach their ends.
All inputs are finite; a program needn't handle non-finite values.
Results may differ from the reference program's by a relative error of at most 0.0055.
Values may be sent and summed in bfloat16 or wider, within the bound.
No kernel may reach another device: no remote copies, remote signals or barrier semaphores. Data moves between devices by JAX's collectives and lax.ppermute only.
A program may use at most 192 MiB of HBM per device.

```python
import math
import jax
import jax.numpy as jnp
import numpy as np

D = 4096
F = 16384
NQ = 4
TQ = 32
WIN = 6
R = 32
SPAN = 128
LAYERS = 4
NSEQ = 64


def set_ends(drawn, stream_key, least, largest):
    spot = [jax.random.randint(jax.random.fold_in(stream_key, axis), (), 0, length) for axis, length in enumerate(drawn.shape)]
    widest = drawn.shape.index(max(drawn.shape))
    next_to = spot[:widest] + [(spot[widest] + 1) % drawn.shape[widest]] + spot[widest + 1:]
    return drawn.at[tuple(spot)].set(least).at[tuple(next_to)].set(largest)


def steps_of(own_key, extent, pieces, low, top_value):
    level, own = 1.0, jax.random.fold_in(own_key, 6)
    for axis_at, blocks in pieces:
        heights = jnp.exp(jax.random.uniform(jax.random.fold_in(own, axis_at), (blocks,), jnp.float32, low / len(pieces), top_value / len(pieces)))
        level = level * jnp.repeat(heights, extent[axis_at] // blocks).reshape([-1 if axis == axis_at else 1 for axis in range(len(extent))])
    return level


def cumulative_ranks(number_of, slope):
    portions = [(1 << 20) // math.isqrt(grade ** slope) + 1 for grade in range(1, number_of + 1)]
    spread = 1 + sum(portions) // (1 << 30)
    return np.cumsum(np.array([max(1, weight // spread) for weight in portions]))


def ranked(key, shape, number_of, lean):
    grid = cumulative_ranks(number_of, lean)
    pick = jax.random.randint(jax.random.fold_in(key, 1), shape, 0, int(grid[number_of - 1]))
    standing = jnp.searchsorted(jnp.asarray(grid, jnp.int32), pick, side="right")
    return jax.random.permutation(jax.random.fold_in(key, 2), number_of)[standing].astype(jnp.int32)


def normal_values(own_key, shape, width, limit, shards=(), kind=jnp.bfloat16):
    level = steps_of(own_key, shape, shards, -0.22, 0.18) if shards else 1.0
    values = jax.random.normal(own_key, shape, jnp.float32) * width * level
    return jnp.minimum(jnp.maximum(values, -limit), limit).astype(kind)


def setup_inputs(seed: int = 0) -> dict:
    keys = jax.random.split(jax.random.key(seed), 10)
    return {
        "out_grads": normal_values(keys[0], (LAYERS, NQ * TQ, F), 0.5, 3.0, ((0, 4), (2, 32))),
        "in_acts": normal_values(keys[1], (LAYERS, NQ * TQ, D), 0.5, 3.0, ((0, 4), (2, 32))),
        "out_basis": normal_values(keys[2], (LAYERS, F, F), F ** -0.5, 0.046875, ((0, 4), (2, 32))),
        "in_basis": normal_values(keys[3], (LAYERS, D, D), D ** -0.5, 0.09375, ((0, 4), (2, 32))),
        "eigenvalues": jnp.clip(jnp.exp(math.log(50.0) - 4.6051702 * jax.random.uniform(keys[4], (LAYERS, F, D), jnp.float32) ** steps_of(keys[4], (LAYERS, F, D), ((0, 4), (1, 32)), -0.2, 0.2)), 0.5, 50.0).astype(jnp.bfloat16),
        "out_store": normal_values(keys[5], (LAYERS, NSEQ, R, F), F ** -0.5, 0.046875, ((0, 4), (1, 32))),
        "in_store": normal_values(keys[6], (LAYERS, NSEQ, R, D), D ** -0.5, 0.09375, ((0, 4), (1, 32))),
        "counts": set_ends(jax.random.randint(keys[7], (NSEQ,), 1, R * SPAN + 1), jax.random.fold_in(keys[7], 1), 1, R * SPAN).astype(jnp.int32),
        "winners": set_ends(ranked(keys[8], (NQ, WIN), NSEQ, 2), jax.random.fold_in(keys[8], 3), 0, NSEQ - 1).astype(jnp.int32),
    }


damping = 0.1


def reference(out_grads, in_acts, out_basis, in_basis, eigenvalues, out_store, in_store, counts, winners):
    alive = (jnp.arange(R, dtype=jnp.int32)[None, :] * SPAN < counts[:, None]).astype(jnp.bfloat16)
    totals = jnp.zeros((NQ, WIN * R), jnp.float32)
    for layer_index in range(LAYERS):
        turned_out = jnp.dot(out_grads[layer_index], out_basis[layer_index], preferred_element_type=jnp.float32).astype(jnp.bfloat16)
        turned_in = jnp.dot(in_acts[layer_index], in_basis[layer_index], preferred_element_type=jnp.float32).astype(jnp.bfloat16)
        masked = in_store[layer_index] * alive[:, :, None]
        divisor = eigenvalues[layer_index].astype(jnp.float32) + damping
        for query_index in range(NQ):
            left = turned_out[query_index * TQ:(query_index + 1) * TQ]
            right = turned_in[query_index * TQ:(query_index + 1) * TQ]
            product = jnp.dot(left.T, right, preferred_element_type=jnp.float32)
            precond = (product / divisor).astype(jnp.bfloat16)
            chosen = winners[query_index]
            right_rows = masked[chosen].reshape(WIN * R, D)
            left_rows = out_store[layer_index][chosen].reshape(WIN * R, F)
            mapped = jnp.dot(precond, right_rows.T, preferred_element_type=jnp.float32)
            terms = jnp.sum(mapped.T * left_rows.astype(jnp.float32), axis=1)
            totals = totals.at[query_index].add(terms)
    return totals.reshape(NQ, WIN, R)
```

```python
import jax
import jax.numpy as jnp
import numpy as np
from jax import lax
from jax.experimental import pallas as pl
from jax.experimental.pallas import tpu as pltpu
from jax.sharding import Mesh
from jax.sharding import PartitionSpec as P


NQ = 4
TQ = 32
WIN = 6
R = 32
SPAN = 128
Y, Z, X = "dp_0", "dp_1", "dp_2"
DP = (Y, Z, X)
LAYER = ("layer_0", "layer_1")
LANES = 128
PER_Q = WIN * R

damping = 0.1


def shifted(value, axis, step):
    count = lax.axis_size(axis)
    return lax.ppermute(value, axis, [(i, (i + step) % count) for i in range(count)])


def far_of(before, after, axis):
    half = before.shape[0] // 2
    low = shifted(before[:half], axis, 1)
    high = shifted(after[half:], axis, -1)
    return jnp.concatenate([low, high], axis=0)


def orders(y, z, x, core):
    ring = np.array([0, 3, 1, 2], np.int32)
    pair = np.array([0, 1], np.int32)
    ys, xs = (y + ring) % 4, (x + ring) % 4
    turn = ys[None, :, None] * 8 + ((z + pair) % 2)[None, None, :] * 4 + xs[:, None, None]
    inner = (((core + pair) % 2)[:, None] * 4 + xs[None, :]).reshape(1, 8)
    maps = jnp.concatenate([jnp.broadcast_to(inner, (4, 8)), ys[:, None]], axis=1).reshape(-1)
    own = jnp.where(core == z, 1, 0).reshape(1)
    return turn.reshape(-1).astype(jnp.int32), jnp.concatenate([maps, own]).astype(jnp.int32)


def received(value):
    return lax.ppermute(value, ("layer_1", Z), [(1, 2), (2, 1)])


def traded(value):
    same = lax.axis_index("layer_1") == lax.axis_index(Z)
    return jnp.where(same, value, received(value))


def pack_first(counts, in_acts, in_store):
    rows, width = in_store.shape
    t = in_acts.shape[0]
    count = width // LANES
    step = 8

    def body(counts_ref, acts_ref, store_ref, out_ref):
        row = lax.broadcasted_iota(jnp.int32, (rows, LANES), 0)
        start = (row % R) * SPAN
        alive = start < jnp.where(row < R, counts_ref[0], counts_ref[1])
        for j in range(step):
            out_ref[j, :t, :] = acts_ref[...]
            part = store_ref[:, j * LANES : (j + 1) * LANES].astype(jnp.float32)
            out_ref[j, t:, :] = jnp.where(alive, part, 0.0).astype(jnp.bfloat16)

    return pl.pallas_call(
        body,
        grid_spec=pltpu.PrefetchScalarGridSpec(
            num_scalar_prefetch=1,
            grid=(count // step,),
            in_specs=[
                pl.BlockSpec((t, LANES), lambda i, c: (0, 0)),
                pl.BlockSpec((rows, step * LANES), lambda i, c: (0, i)),
            ],
            out_specs=pl.BlockSpec((step, t + rows, LANES), lambda i, c: (i, 0, 0)),
        ),
        out_shape=jax.ShapeDtypeStruct((count, t + rows, LANES), jnp.bfloat16),
        name="pack_first",
    )(counts, in_acts, in_store)


def pack_left(store, width):
    rows, full = store.shape
    count = full // width
    step = 4

    def body(store_ref, out_ref):
        for j in range(step):
            out_ref[j] = store_ref[:, j * width : (j + 1) * width]

    return pl.pallas_call(
        body,
        grid=(count // step,),
        in_specs=[pl.BlockSpec((rows, step * width), lambda i: (0, i))],
        out_specs=pl.BlockSpec((step, rows, width), lambda i: (i, 0, 0)),
        out_shape=jax.ShapeDtypeStruct((count, rows, width), jnp.bfloat16),
        name="pack_left",
    )(store)


def head(winners, first, basis, t):
    sources, _, lanes = first.shape
    count = winners.shape[0]

    def body(winners_ref, first_ref, basis_ref, out_ref):
        for i in range(count):
            n = winners_ref[i]
            at = pl.multiple_of(t + n % 2 * R, R)
            out_ref[i * R : (i + 1) * R, :] = first_ref[n // 2, pl.ds(at, R), :]
        turned = jnp.zeros((t, lanes), jnp.float32)
        for s in range(0, sources, 2):
            acts = jnp.concatenate([first_ref[s, :t, :], first_ref[s + 1, :t, :]], axis=1)
            turned += jnp.dot(
                acts,
                basis_ref[s * lanes : (s + 2) * lanes, :],
                preferred_element_type=jnp.float32,
            )
        out_ref[count * R :, :] = turned.astype(jnp.bfloat16)

    return pl.pallas_call(
        body,
        grid_spec=pltpu.PrefetchScalarGridSpec(
            num_scalar_prefetch=1,
            grid=(1,),
            in_specs=[
                pl.BlockSpec(first.shape, lambda i, w: (0, 0, 0)),
                pl.BlockSpec(basis.shape, lambda i, w: (0, 0)),
            ],
            out_specs=pl.BlockSpec((count * R + t, lanes), lambda i, w: (0, 0)),
        ),
        out_shape=jax.ShapeDtypeStruct((count * R + t, lanes), jnp.bfloat16),
        name="head",
    )(winners, first, basis)


def turn_part(group, value, order, basis, total):
    blocks, rows, width = value.shape
    out_width = basis.shape[1]
    step = 4
    final = group == 3

    def body(order_ref, value_ref, *refs):
        basis_refs, rest = refs[:step], refs[step:]
        out_ref, sum_ref = rest[-2:]

        @pl.when(pl.program_id(0) == 0)
        def _():
            sum_ref[...] = rest[0][...] if total is not None else jnp.zeros_like(sum_ref)

        part = sum_ref[...]
        for j in range(step):
            part = part + jnp.dot(
                value_ref[j], basis_refs[j][...], preferred_element_type=jnp.float32
            )
        sum_ref[...] = part

        @pl.when(pl.program_id(0) == blocks // step - 1)
        def _():
            out_ref[...] = part.astype(out_ref.dtype)

    whole = pl.BlockSpec((rows, out_width), lambda i, o: (0, 0))
    return pl.pallas_call(
        body,
        grid_spec=pltpu.PrefetchScalarGridSpec(
            num_scalar_prefetch=1,
            grid=(blocks // step,),
            in_specs=[pl.BlockSpec((step, rows, width), lambda i, o: (i, 0, 0))]
            + [
                pl.BlockSpec(
                    (width, out_width), lambda i, o, j=j: (o[group * blocks + i * step + j], 0)
                )
                for j in range(step)
            ]
            + ([] if total is None else [whole]),
            out_specs=whole,
            scratch_shapes=[pltpu.VMEM((rows, out_width), jnp.float32)],
        ),
        out_shape=jax.ShapeDtypeStruct((rows, out_width), jnp.bfloat16 if final else jnp.float32),
        cost_estimate=pl.CostEstimate(
            flops=2 * blocks * width * rows * out_width,
            bytes_accessed=2 * blocks * width * out_width,
            transcendentals=0,
        ),
        name="turn_part",
    )(order, value, *[basis] * step, *([] if total is None else [total]))


def map_part(group, parts, order, eigens, left, total, left_rows):
    blocks = parts[0].shape[0]
    out_width = eigens[0].shape[0]
    count = 2 * blocks
    columns = count * LANES
    base = group * (count + 1)
    own_at = 4 * (count + 1)
    tile = 256
    final = group == 3

    def body(order_ref, near_ref, far_ref, own_ref, got_ref, left_ref, *refs):
        out_ref = refs[-1]

        def rows_of(start, size):
            pieces = [r[b, start : start + size, :] for r in (near_ref, far_ref) for b in range(blocks)]
            return jnp.concatenate(pieces, axis=1)

        def eigen_of(b):
            at = pl.multiple_of(order_ref[base + b] * LANES, LANES)
            own, got = (r[:, pl.ds(at, LANES)].astype(jnp.float32) for r in (own_ref, got_ref))
            return jnp.where(order_ref[own_at] == 1, own, got)

        scale = jnp.concatenate([eigen_of(b) for b in range(count)], axis=1)
        scale = 1.0 / (scale + damping)
        for q in range(NQ):
            product = lax.dot_general(
                left_ref[q * TQ : (q + 1) * TQ, :],
                rows_of(NQ * PER_Q + q * TQ, TQ),
                (((0,), (0,)), ((), ())),
                preferred_element_type=jnp.float32,
            )
            precond = (product * scale).astype(jnp.bfloat16)
            mapped = lax.dot_general(
                precond,
                rows_of(q * PER_Q, PER_Q),
                (((1,), (1,)), ((), ())),
                preferred_element_type=jnp.float32,
            )
            if total is not None:
                mapped = mapped + refs[0][q]
            if final:
                terms = jnp.sum(mapped * refs[1][q].astype(jnp.float32), axis=0, keepdims=True)

                @pl.when(pl.program_id(0) == 0)
                def _():
                    out_ref[q : q + 1, :] = terms

                @pl.when(pl.program_id(0) != 0)
                def _():
                    out_ref[q : q + 1, :] += terms
            else:
                out_ref[q] = mapped

    def own_at_step(i, o):
        return i * o[own_at], o[base + count] * o[own_at]

    def got_at_step(i, o):
        return i * (1 - o[own_at]), 0

    tall = pl.BlockSpec((NQ, tile, PER_Q), lambda i, o: (0, i, 0))
    in_specs = [pl.BlockSpec(p.shape, lambda i, o: (0, 0, 0)) for p in parts]
    in_specs += [
        pl.BlockSpec((tile, columns), own_at_step),
        pl.BlockSpec((tile, columns), got_at_step),
        pl.BlockSpec((NQ * TQ, tile), lambda i, o: (0, i)),
    ]
    operands = [*parts, *eigens, left]
    if total is not None:
        in_specs.append(tall)
        operands.append(total)
    if final:
        in_specs.append(tall)
        operands.append(left_rows)
        out_shape = jax.ShapeDtypeStruct((NQ, PER_Q), jnp.float32)
        out_spec = pl.BlockSpec((NQ, PER_Q), lambda i, o: (0, 0))
    else:
        out_shape = jax.ShapeDtypeStruct((NQ, out_width, PER_Q), jnp.float32)
        out_spec = tall
    return pl.pallas_call(
        body,
        grid_spec=pltpu.PrefetchScalarGridSpec(
            num_scalar_prefetch=1,
            grid=(out_width // tile,),
            in_specs=in_specs,
            out_specs=out_spec,
        ),
        out_shape=out_shape,
        cost_estimate=pl.CostEstimate(
            flops=2 * NQ * out_width * columns * (PER_Q + 8 * TQ),
            bytes_accessed=2 * out_width * columns,
            transcendentals=0,
        ),
        name="map_part",
    )(order, *operands)


def sum_everywhere(value):
    for axis in ("layer_1", Z, "layer_0", Y, X):
        if lax.axis_size(axis) == 2:
            value = value + shifted(value, axis, 1)
        else:
            far, before, after = (shifted(value, axis, step) for step in (2, 1, 3))
            value = (value + far) + (before + after)
    return value


def on_device(
    out_grads, in_acts, out_basis, in_basis, eigenvalues, out_store, in_store, counts, winners
):
    y, z, x = (lax.axis_index(a) for a in DP)
    out_width = out_basis.shape[2]
    out_full = out_basis.shape[1]
    in_full = in_basis.shape[1]
    t = out_grads.shape[1]
    chosen = winners.reshape(NQ * WIN)

    turn_order, map_order = orders(y, z, x, lax.axis_index("layer_1"))

    own = eigenvalues[0]
    quarter = in_full // 4
    got = []
    for group in range(4):
        part = lax.dynamic_slice_in_dim(own, map_order[9 * group + 8] * quarter, quarter, 1)
        got.append(received(part))

    packed = pack_first(counts, in_acts[0], in_store[0].reshape(-1, in_full))
    first = lax.all_to_all(packed, DP, 0, 0, tiled=True)

    grads = out_grads[0]
    grads = jnp.stack([grads, shifted(grads, Z, 1)])
    g_before, g_after = shifted(grads, Y, 1), shifted(grads, Y, -1)
    g_far = far_of(g_before, g_after, Y)
    grads = jnp.concatenate([grads, g_before, g_after, g_far], axis=0)
    g_before, g_after = shifted(grads, X, 1), shifted(grads, X, -1)
    total = turn_part(0, grads, turn_order, out_basis[0], None)
    g_far = far_of(g_before, g_after, X)
    total = turn_part(1, g_before, turn_order, out_basis[0], total)
    total = turn_part(2, g_after, turn_order, out_basis[0], total)
    left = traded(turn_part(3, g_far, turn_order, out_basis[0], total))

    both = head(chosen, first, in_basis[0], t)
    both = traded(both)
    both = [both, *(shifted(both, X, s) for s in (1, -1, 2))]
    both = jnp.stack(both)
    b_before, b_after = shifted(both, Y, 1), shifted(both, Y, -1)
    b_far = far_of(b_before, b_after, Y)

    store = pack_left(out_store[0].reshape(-1, out_full), out_width)
    slices = lax.all_to_all(store, DP, 0, 0, tiled=True)
    left_rows = jnp.take(slices.reshape(-1, R, out_width), chosen, axis=0)
    left_rows = traded(left_rows.reshape(NQ, PER_Q, out_width).transpose(0, 2, 1))

    mapped = None
    for group, part in enumerate((both, b_before, b_after, b_far)):
        parts = (part, shifted(part, "layer_1", 1))
        mapped = map_part(group, parts, map_order, (own, got[group]), left, mapped, left_rows)
    totals = sum_everywhere(mapped.reshape(-1, LANES))
    return totals.reshape(NQ, WIN, R)


def solution(mesh):
    torus = Mesh(
        mesh.devices.reshape(2, 2, 4, 2, 4), ("layer_0", "layer_1", "dp_0", "dp_1", "dp_2")
    )
    return jax.shard_map(
        on_device,
        mesh=torus,
        in_specs=(
            P(LAYER, None, DP),
            P(LAYER, None, DP),
            P(LAYER, None, DP),
            P(LAYER, None, DP),
            P(LAYER, DP, None),
            P(LAYER, DP, None, None),
            P(LAYER, DP, None, None),
            P(DP),
            P(),
        ),
        out_specs=P(),
        check_vma=False,
    )
```

```python
import jax
import jax.numpy as jnp
import numpy as np
from jax import lax
from jax.experimental import pallas as pl
from jax.experimental.pallas import tpu as pltpu
from jax.sharding import Mesh
from jax.sharding import PartitionSpec as P


NQ = 4
TQ = 32
WIN = 6
R = 32
SPAN = 128
Y, Z, X = "dp_0", "dp_1", "dp_2"
DP = (Y, Z, X)
LAYER = ("layer_0", "layer_1")
LANES = 128
PER_Q = WIN * R

damping = 0.1


def shifted(value, axis, step):
    count = lax.axis_size(axis)
    return lax.ppermute(value, axis, [(i, (i + step) % count) for i in range(count)])


def far_of(before, after, axis):
    half = before.shape[0] // 2
    low = shifted(before[:half], axis, 1)
    high = shifted(after[half:], axis, -1)
    return jnp.concatenate([low, high], axis=0)


def orders(y, z, x, core):
    ring = np.array([0, 3, 1, 2], np.int32)
    pair = np.array([0, 1], np.int32)
    ys, xs = (y + ring) % 4, (x + ring) % 4
    turn = ys[None, :, None] * 8 + ((z + pair) % 2)[None, None, :] * 4 + xs[:, None, None]
    inner = (((core + pair) % 2)[:, None] * 4 + xs[None, :]).reshape(1, 8)
    maps = jnp.concatenate([jnp.broadcast_to(inner, (4, 8)), ys[:, None]], axis=1).reshape(-1)
    own = jnp.where(core == z, 1, 0).reshape(1)
    return turn.reshape(-1).astype(jnp.int32), jnp.concatenate([maps, own]).astype(jnp.int32)


def received(value):
    return lax.ppermute(value, ("layer_1", Z), [(1, 2), (2, 1)])


def traded(value):
    same = lax.axis_index("layer_1") == lax.axis_index(Z)
    return jnp.where(same, value, received(value))


def pack_first(counts, in_acts, in_store):
    rows, width = in_store.shape
    t = in_acts.shape[0]
    count = width // LANES
    step = 8

    def body(counts_ref, acts_ref, store_ref, out_ref):
        row = lax.broadcasted_iota(jnp.int32, (rows, LANES), 0)
        start = (row % R) * SPAN
        alive = start < jnp.where(row < R, counts_ref[0], counts_ref[1])
        for j in range(step):
            out_ref[j, :t, :] = acts_ref[...]
            part = store_ref[:, j * LANES : (j + 1) * LANES].astype(jnp.float32)
            out_ref[j, t:, :] = jnp.where(alive, part, 0.0).astype(jnp.bfloat16)

    return pl.pallas_call(
        body,
        grid_spec=pltpu.PrefetchScalarGridSpec(
            num_scalar_prefetch=1,
            grid=(count // step,),
            in_specs=[
                pl.BlockSpec((t, LANES), lambda i, c: (0, 0)),
                pl.BlockSpec((rows, step * LANES), lambda i, c: (0, i)),
            ],
            out_specs=pl.BlockSpec((step, t + rows, LANES), lambda i, c: (i, 0, 0)),
        ),
        out_shape=jax.ShapeDtypeStruct((count, t + rows, LANES), jnp.bfloat16),
        name="pack_first",
    )(counts, in_acts, in_store)


def cut_columns(map_order, value):
    rows, full = value.shape
    groups = 4
    width, tile = full // groups, 128

    def body(order_ref, *refs):
        for g in range(groups):
            refs[groups + g][...] = refs[g][...]

    return pl.pallas_call(
        body,
        grid_spec=pltpu.PrefetchScalarGridSpec(
            num_scalar_prefetch=1,
            grid=(rows // tile,),
            in_specs=[
                pl.BlockSpec((tile, width), lambda i, o, g=g: (i, o[9 * g + 8]))
                for g in range(groups)
            ],
            out_specs=[pl.BlockSpec((tile, width), lambda i, o: (i, 0))] * groups,
        ),
        out_shape=[jax.ShapeDtypeStruct((rows, width), value.dtype)] * groups,
        name="cut_columns",
    )(map_order, *[value] * groups)


def pack_left(store, width):
    rows, full = store.shape
    count = full // width
    step = 4

    def body(store_ref, out_ref):
        for j in range(step):
            out_ref[j] = store_ref[:, j * width : (j + 1) * width]

    return pl.pallas_call(
        body,
        grid=(count // step,),
        in_specs=[pl.BlockSpec((rows, step * width), lambda i: (0, i))],
        out_specs=pl.BlockSpec((step, rows, width), lambda i: (i, 0, 0)),
        out_shape=jax.ShapeDtypeStruct((count, rows, width), jnp.bfloat16),
        name="pack_left",
    )(store)


def head(winners, first, basis, t):
    sources, _, lanes = first.shape
    count = winners.shape[0]

    def body(winners_ref, first_ref, basis_ref, out_ref):
        for i in range(count):
            n = winners_ref[i]
            at = pl.multiple_of(t + n % 2 * R, R)
            out_ref[i * R : (i + 1) * R, :] = first_ref[n // 2, pl.ds(at, R), :]
        turned = jnp.zeros((t, lanes), jnp.float32)
        for s in range(0, sources, 2):
            acts = jnp.concatenate([first_ref[s, :t, :], first_ref[s + 1, :t, :]], axis=1)
            turned += jnp.dot(
                acts,
                basis_ref[s * lanes : (s + 2) * lanes, :],
                preferred_element_type=jnp.float32,
            )
        out_ref[count * R :, :] = turned.astype(jnp.bfloat16)

    return pl.pallas_call(
        body,
        grid_spec=pltpu.PrefetchScalarGridSpec(
            num_scalar_prefetch=1,
            grid=(1,),
            in_specs=[
                pl.BlockSpec(first.shape, lambda i, w: (0, 0, 0)),
                pl.BlockSpec(basis.shape, lambda i, w: (0, 0)),
            ],
            out_specs=pl.BlockSpec((count * R + t, lanes), lambda i, w: (0, 0)),
        ),
        out_shape=jax.ShapeDtypeStruct((count * R + t, lanes), jnp.bfloat16),
        name="head",
    )(winners, first, basis)


def turn_part(group, value, order, basis, total):
    blocks, rows, width = value.shape
    out_width = basis.shape[1]
    step = 4
    final = group == 3

    def body(order_ref, value_ref, *refs):
        basis_refs, rest = refs[:step], refs[step:]
        out_ref, sum_ref = rest[-2:]

        @pl.when(pl.program_id(0) == 0)
        def _():
            sum_ref[...] = rest[0][...] if total is not None else jnp.zeros_like(sum_ref)

        part = sum_ref[...]
        for j in range(step):
            part = part + jnp.dot(
                value_ref[j], basis_refs[j][...], preferred_element_type=jnp.float32
            )
        sum_ref[...] = part

        @pl.when(pl.program_id(0) == blocks // step - 1)
        def _():
            out_ref[...] = part.astype(out_ref.dtype)

    whole = pl.BlockSpec((rows, out_width), lambda i, o: (0, 0))
    return pl.pallas_call(
        body,
        grid_spec=pltpu.PrefetchScalarGridSpec(
            num_scalar_prefetch=1,
            grid=(blocks // step,),
            in_specs=[pl.BlockSpec((step, rows, width), lambda i, o: (i, 0, 0))]
            + [
                pl.BlockSpec(
                    (width, out_width), lambda i, o, j=j: (o[group * blocks + i * step + j], 0)
                )
                for j in range(step)
            ]
            + ([] if total is None else [whole]),
            out_specs=whole,
            scratch_shapes=[pltpu.VMEM((rows, out_width), jnp.float32)],
        ),
        out_shape=jax.ShapeDtypeStruct((rows, out_width), jnp.bfloat16 if final else jnp.float32),
        cost_estimate=pl.CostEstimate(
            flops=2 * blocks * width * rows * out_width,
            bytes_accessed=2 * blocks * width * out_width,
            transcendentals=0,
        ),
        name="turn_part",
    )(order, value, *[basis] * step, *([] if total is None else [total]))


def map_part(group, parts, order, eigens, left, total, left_rows):
    blocks = parts[0].shape[0]
    out_width = eigens[0].shape[0]
    count = 2 * blocks
    columns = count * LANES
    base = group * (count + 1)
    own_at = 4 * (count + 1)
    tile = 256
    final = group == 3

    def body(order_ref, near_ref, far_ref, own_ref, got_ref, left_ref, *refs):
        out_ref = refs[-1]

        def rows_of(start, size):
            pieces = [r[b, start : start + size, :] for r in (near_ref, far_ref) for b in range(blocks)]
            return jnp.concatenate(pieces, axis=1)

        def eigen_of(b):
            at = pl.multiple_of(order_ref[base + b] * LANES, LANES)
            own, got = (r[:, pl.ds(at, LANES)].astype(jnp.float32) for r in (own_ref, got_ref))
            return jnp.where(order_ref[own_at] == 1, own, got)

        scale = jnp.concatenate([eigen_of(b) for b in range(count)], axis=1)
        scale = 1.0 / (scale + damping)
        for q in range(NQ):
            product = lax.dot_general(
                left_ref[q * TQ : (q + 1) * TQ, :],
                rows_of(NQ * PER_Q + q * TQ, TQ),
                (((0,), (0,)), ((), ())),
                preferred_element_type=jnp.float32,
            )
            precond = (product * scale).astype(jnp.bfloat16)
            mapped = lax.dot_general(
                precond,
                rows_of(q * PER_Q, PER_Q),
                (((1,), (1,)), ((), ())),
                preferred_element_type=jnp.float32,
            )
            if total is not None:
                mapped = mapped + refs[0][q]
            if final:
                terms = jnp.sum(mapped * refs[1][q].astype(jnp.float32), axis=0, keepdims=True)

                @pl.when(pl.program_id(0) == 0)
                def _():
                    out_ref[q : q + 1, :] = terms

                @pl.when(pl.program_id(0) != 0)
                def _():
                    out_ref[q : q + 1, :] += terms
            else:
                out_ref[q] = mapped

    def own_at_step(i, o):
        return i * o[own_at], o[base + count] * o[own_at]

    def got_at_step(i, o):
        return i * (1 - o[own_at]), 0

    tall = pl.BlockSpec((NQ, tile, PER_Q), lambda i, o: (0, i, 0))
    in_specs = [pl.BlockSpec(p.shape, lambda i, o: (0, 0, 0)) for p in parts]
    in_specs += [
        pl.BlockSpec((tile, columns), own_at_step),
        pl.BlockSpec((tile, columns), got_at_step),
        pl.BlockSpec((NQ * TQ, tile), lambda i, o: (0, i)),
    ]
    operands = [*parts, *eigens, left]
    if total is not None:
        in_specs.append(tall)
        operands.append(total)
    if final:
        in_specs.append(tall)
        operands.append(left_rows)
        out_shape = jax.ShapeDtypeStruct((NQ, PER_Q), jnp.float32)
        out_spec = pl.BlockSpec((NQ, PER_Q), lambda i, o: (0, 0))
    else:
        out_shape = jax.ShapeDtypeStruct((NQ, out_width, PER_Q), jnp.float32)
        out_spec = tall
    return pl.pallas_call(
        body,
        grid_spec=pltpu.PrefetchScalarGridSpec(
            num_scalar_prefetch=1,
            grid=(out_width // tile,),
            in_specs=in_specs,
            out_specs=out_spec,
        ),
        out_shape=out_shape,
        cost_estimate=pl.CostEstimate(
            flops=2 * NQ * out_width * columns * (PER_Q + 8 * TQ),
            bytes_accessed=2 * out_width * columns,
            transcendentals=0,
        ),
        name="map_part",
    )(order, *operands)


def sum_everywhere(value):
    for axis in ("layer_1", Z, "layer_0", Y, X):
        if lax.axis_size(axis) == 2:
            value = value + shifted(value, axis, 1)
        else:
            far, before, after = (shifted(value, axis, step) for step in (2, 1, 3))
            value = (value + far) + (before + after)
    return value


def on_device(
    out_grads, in_acts, out_basis, in_basis, eigenvalues, out_store, in_store, counts, winners
):
    y, z, x = (lax.axis_index(a) for a in DP)
    out_width = out_basis.shape[2]
    out_full = out_basis.shape[1]
    in_full = in_basis.shape[1]
    t = out_grads.shape[1]
    chosen = winners.reshape(NQ * WIN)

    turn_order, map_order = orders(y, z, x, lax.axis_index("layer_1"))

    own = eigenvalues[0]
    parts = cut_columns(map_order, own)
    got = [received(part) for part in parts]

    packed = pack_first(counts, in_acts[0], in_store[0].reshape(-1, in_full))
    first = lax.all_to_all(packed, DP, 0, 0, tiled=True)

    grads = out_grads[0]
    grads = jnp.stack([grads, shifted(grads, Z, 1)])
    g_before, g_after = shifted(grads, Y, 1), shifted(grads, Y, -1)
    g_far = far_of(g_before, g_after, Y)
    grads = jnp.concatenate([grads, g_before, g_after, g_far], axis=0)
    g_before, g_after = shifted(grads, X, 1), shifted(grads, X, -1)
    total = turn_part(0, grads, turn_order, out_basis[0], None)
    g_far = far_of(g_before, g_after, X)
    total = turn_part(1, g_before, turn_order, out_basis[0], total)
    total = turn_part(2, g_after, turn_order, out_basis[0], total)
    left = traded(turn_part(3, g_far, turn_order, out_basis[0], total))

    both = head(chosen, first, in_basis[0], t)
    both = traded(both)
    both = [both, *(shifted(both, X, s) for s in (1, -1, 2))]
    both = jnp.stack(both)
    b_before, b_after = shifted(both, Y, 1), shifted(both, Y, -1)
    b_far = far_of(b_before, b_after, Y)

    store = pack_left(out_store[0].reshape(-1, out_full), out_width)
    slices = lax.all_to_all(store, DP, 0, 0, tiled=True)
    left_rows = jnp.take(slices.reshape(-1, R, out_width), chosen, axis=0)
    left_rows = traded(left_rows.reshape(NQ, PER_Q, out_width).transpose(0, 2, 1))

    mapped = None
    for group, part in enumerate((both, b_before, b_after, b_far)):
        parts = (part, shifted(part, "layer_1", 1))
        eigens = (own, got[group])
        mapped = map_part(group, parts, map_order, eigens, left, mapped, left_rows)
    totals = sum_everywhere(mapped.reshape(-1, LANES))
    return totals.reshape(NQ, WIN, R)


def solution(mesh):
    torus = Mesh(
        mesh.devices.reshape(2, 2, 4, 2, 4), ("layer_0", "layer_1", "dp_0", "dp_1", "dp_2")
    )
    return jax.shard_map(
        on_device,
        mesh=torus,
        in_specs=(
            P(LAYER, None, DP),
            P(LAYER, None, DP),
            P(LAYER, None, DP),
            P(LAYER, None, DP),
            P(LAYER, DP, None),
            P(LAYER, DP, None, None),
            P(LAYER, DP, None, None),
            P(DP),
            P(),
        ),
        out_specs=P(),
        check_vma=False,
    )
```
